32 devices in a mesh: rep: 8 (over z, x), shard: 4 (over y, core).
Axes of the slice: x: 2, y: 2, z: 4, core: 2. Of those that a mesh axis runs over, the one named last changes fastest.
Arguments:
- inputs: bfloat16 [2560, 4096], P('rep', 'shard'), may hold values from -6 to 6
- weight: float32 [4096, 4096], P('shard', 'rep'), may hold values from -0.09375 to 0.09375
- table: bfloat16 [256, 4096], replicated, may hold values from -6 to 6
- targets: int32 [2560], P(('rep', 'shard')), may hold values from 0 to 255
Outputs:
- combined: float32 [4096, 4096], P('shard', 'rep')
- new_weight: float32 [4096, 4096], P('shard', 'rep')
The draws below stay inside these ranges and needn't reach their ends.
All inputs are finite; a program needn't handle non-finite values.
Results may differ from the reference program's by a relative error of at most 0.005.
Values may be sent and summed in bfloat16 or wider, within the bound.
No kernel may reach another device: no remote copies, remote signals or barrier semaphores. Data moves between devices by JAX's collectives and lax.ppermute only.
A program may use at most 128 MiB of HBM per device.

```python
import math
import jax
import jax.numpy as jnp
import numpy as np
from jax import lax

D = 4096
NBEST = 256
ROWS = 320
ALL_ROWS = 2560
N_REP = 8


def place_ends(array, rng, low, top_value):
    longest = array.shape.index(max(array.shape))
    spots = []
    for shift in (0, 1):
        where = [jax.random.randint(jax.random.fold_in(rng, axis), (), 0, length) for axis, length in enumerate(array.shape)]
        where[longest] = (where[longest] + shift) % array.shape[longest]
        spots.append(tuple(where))
    return array.at[spots[0]].set(low).at[spots[1]].set(top_value)


def level_of(rng, shape, pieces, low, top_value):
    level = 1.0
    for position, shards_of in pieces:
        draws = jax.random.uniform(jax.random.fold_in(jax.random.fold_in(rng, 6), position), (shards_of,), jnp.float32, low / len(pieces), top_value / len(pieces))
        level = level * jnp.repeat(jnp.exp(draws), shape[position] // shards_of).reshape((-1,) + (1,) * (len(shape) - 1 - position))
    return level


def rank_table(amount, lean):
    loads = [(1 << 20) // math.isqrt(grade ** lean) + 1 for grade in range(1, amount + 1)]
    spread = 1 + sum(loads) // (1 << 30)
    return np.cumsum(np.array([max(1, weight // spread) for weight in loads]))


def ranked_ids(stream_key, dims, count, slope):
    table = rank_table(count, slope)
    pick = jax.random.randint(jax.random.fold_in(stream_key, 1), dims, 0, int(table[count - 1]))
    rank = jnp.searchsorted(jnp.asarray(table, jnp.int32), pick, side="right")
    return jax.random.permutation(jax.random.fold_in(stream_key, 2), count)[rank].astype(jnp.int32)


def normal_values(key, extent, scale, bound, pieces=(), dtype=jnp.bfloat16):
    values = scale * jax.random.normal(key, extent, jnp.float32)
    if pieces:
        values = values * level_of(key, extent, pieces, -0.22, 0.18)
    return jnp.clip(values, -bound, bound).astype(dtype)


def setup_inputs(seed: int = 0) -> dict:
    streams_of = jax.random.split(jax.random.key(seed), 5)
    inputs = normal_values(streams_of[0], (ALL_ROWS, D), 1.0, 6.0, ((0, 8), (1, 4)))
    weight = normal_values(streams_of[1], (D, D), D ** -0.5, 0.09375, ((0, 4), (1, 8)), jnp.float32)
    table = normal_values(streams_of[2], (NBEST, D), 1.0, 6.0)
    targets = place_ends(ranked_ids(streams_of[3], (ALL_ROWS,), NBEST, 2), jax.random.fold_in(streams_of[3], 3), 0, NBEST - 1).astype(jnp.int32)
    return dict(inputs=inputs, weight=weight, table=table, targets=targets)


epsilon = 1e-06
step_size = 0.05

def adasum_pair(lower_vec, upper_vec):
    cross = jnp.sum(lower_vec * upper_vec)
    norm_low = jnp.sum(lower_vec * lower_vec)
    norm_high = jnp.sum(upper_vec * upper_vec)
    return (1.0 - cross / (2.0 * (norm_low + epsilon))) * lower_vec + (1.0 - cross / (2.0 * (norm_high + epsilon))) * upper_vec

def replica_grad(replica, inputs, weight_b, table, targets):
    row_block = inputs[replica * ROWS:(replica + 1) * ROWS].astype(jnp.float32)
    outputs = jnp.dot(row_block, weight_b, precision=lax.Precision.HIGHEST)
    wanted = table[targets[replica * ROWS:(replica + 1) * ROWS]].astype(jnp.float32)
    error = ((outputs - wanted) / ROWS).astype(jnp.bfloat16).astype(jnp.float32)
    return jnp.dot(row_block.T, error, precision=lax.Precision.HIGHEST)

def reference(inputs, weight, table, targets):
    weight_b = weight.astype(jnp.bfloat16).astype(jnp.float32)

    def subtree(low_end, high_end):
        if high_end - low_end == 1:
            return replica_grad(low_end, inputs, weight_b, table, targets)
        middle = (low_end + high_end) // 2
        return adasum_pair(subtree(low_end, middle), subtree(middle, high_end))
    combined = subtree(0, N_REP)
    return (combined, weight - step_size * combined)
```

```python
import functools

import jax
import jax.numpy as jnp
from jax import lax
from jax.experimental import pallas as pl
from jax.experimental.pallas import tpu as pltpu
from jax.sharding import PartitionSpec as P

epsilon = 1e-06
step_size = 0.05


def mix_pair(cross, norm_low, norm_high):
    norm_low = jnp.maximum(norm_low, 0.0)
    norm_high = jnp.maximum(norm_high, 0.0)
    bound = jnp.sqrt(norm_low) * jnp.sqrt(norm_high)
    cross = jnp.minimum(jnp.maximum(cross, -bound), bound)
    return (
        1.0 - cross / (2.0 * (norm_low + epsilon)),
        1.0 - cross / (2.0 * (norm_high + epsilon)),
    )


def tree_weights(entry, count):
    products = {(a, b): entry(a, b) for a in range(count) for b in range(a, count)}
    weights = [None] * count
    group = 1
    alive = count
    while alive > 1:
        factors = []
        for m in range(alive // 2):
            low, high = mix_pair(
                products[2 * m, 2 * m + 1], products[2 * m, 2 * m], products[2 * m + 1, 2 * m + 1]
            )
            factors.append((low, high))
            for r in range(2 * m * group, (2 * m + 1) * group):
                weights[r] = low if weights[r] is None else weights[r] * low
            for r in range((2 * m + 1) * group, (2 * m + 2) * group):
                weights[r] = high if weights[r] is None else weights[r] * high
        merged = {}
        for a in range(alive // 2):
            for b in range(a, alive // 2):
                terms = [
                    factors[a][i]
                    * factors[b][j]
                    * products[min(2 * a + i, 2 * b + j), max(2 * a + i, 2 * b + j)]
                    for i in range(2)
                    for j in range(2)
                ]
                merged[a, b] = (terms[0] + terms[3]) + (terms[1] + terms[2])
        products = merged
        alive //= 2
        group *= 2
    return weights


def grad_kernel(*refs, news, olds, halves, tile):
    xs = refs[: news * halves]
    errors = refs[news * halves]
    old = refs[news * halves + 1 : news * halves + 1 + olds]
    new = refs[news * halves + 1 + olds : news * halves + 1 + olds + news]
    sums = refs[-1]

    @pl.when(pl.program_id(0) == 0)
    def _():
        sums[...] = jnp.zeros_like(sums)

    for n in range(news):
        block = jnp.concatenate([xs[n * halves + h][...] for h in range(halves)], axis=0)
        new[n][...] = lax.dot_general(
            block, errors[n], (((0,), (0,)), ((), ())), preferred_element_type=jnp.float32
        )
    every = list(old) + list(new)
    pairs = [(i, olds + n) for n in range(news) for i in range(olds + n + 1)]
    columns = new[0].shape[1] // 128

    def body(step, carry):
        carry = list(carry)
        for c in range(columns):
            got = [ref[pl.ds(pl.multiple_of(step * 8, 8), 8), c * 128 : (c + 1) * 128] for ref in every]
            for k, (i, j) in enumerate(pairs):
                carry[k] = carry[k] + got[i] * got[j]
        return tuple(carry)

    totals = lax.fori_loop(
        0, tile // 8, body, tuple(jnp.zeros((8, 128), jnp.float32) for _ in pairs), unroll=2
    )
    for k in range(len(pairs)):
        sums[k] += totals[k]


def grad_step(xs, halves, errors, old, tile=256):
    news = len(xs) // halves
    features = xs[0].shape[1]
    columns = errors.shape[2]
    olds = len(old)
    pair_count = sum(olds + n + 1 for n in range(news))
    block = pl.BlockSpec((tile, columns), lambda i: (i, 0))
    out = pl.pallas_call(
        functools.partial(grad_kernel, news=news, olds=olds, halves=halves, tile=tile),
        grid=(features // tile,),
        in_specs=[pl.BlockSpec((x.shape[0], tile), lambda i: (0, i)) for x in xs]
        + [pl.BlockSpec(errors.shape, lambda i: (0, 0, 0))]
        + [block] * olds,
        out_specs=[block] * news + [pl.BlockSpec((pair_count, 8, 128), lambda i: (0, 0, 0))],
        out_shape=[jax.ShapeDtypeStruct((features, columns), jnp.float32)] * news
        + [jax.ShapeDtypeStruct((pair_count, 8, 128), jnp.float32)],
        compiler_params=pltpu.CompilerParams(
            dimension_semantics=("arbitrary",), vmem_limit_bytes=16 * 2**20
        ),
        name="grad_%d_%d" % (olds, news),
    )(*xs, errors, *old)
    return out[:news], out[news]


def place_kernel(ids, *refs, pairs):
    out = refs[-1]
    row = lax.broadcasted_iota(jnp.int32, (8, 128), 0)
    column = lax.broadcasted_iota(jnp.int32, (8, 128), 1)
    tile = jnp.zeros((8, 128), jnp.float32)
    at = 0
    for ref in refs[:-1]:
        for k in range(ref.shape[0]):
            i, j = pairs[at]
            at += 1
            total = jnp.sum(ref[k], axis=(0, 1), keepdims=True)
            first, second = ids[i], ids[j]
            here = ((row == first) & (column == second)) | ((row == second) & (column == first))
            tile = jnp.where(here, total, tile)
    out[...] = tile


def combine_kernel(ids, products, weight, *refs, count, tile):
    grads = refs[:count]
    combined, new_weight = refs[count:]
    weights = tree_weights(lambda a, b: jnp.full((8, 128), products[a, b], jnp.float32), count)
    local = []
    for i in range(count):
        value = weights[0]
        for a in range(1, count):
            value = jnp.where(ids[i] == a, weights[a], value)
        local.append(value)
    columns = combined.shape[1] // 128

    def body(step, carry):
        rows = pl.ds(pl.multiple_of(step * 8, 8), 8)
        for c in range(columns):
            lanes = slice(c * 128, (c + 1) * 128)
            total = local[0] * grads[0][rows, lanes]
            for i in range(1, count):
                total = total + local[i] * grads[i][rows, lanes]
            combined[rows, lanes] = total
            new_weight[rows, lanes] = weight[rows, lanes] - step_size * total
        return carry

    lax.fori_loop(0, tile // 8, body, 0, unroll=2)


def ring_path(inputs, weight, table, targets):
    count = lax.axis_size("rep")
    rows = inputs.shape[0]
    features, columns = weight.shape
    rep = lax.axis_index("rep")
    shard = lax.axis_index("shard")
    half = rows // 2
    quarter = rows // 4
    ring = [r for r in range(0, count, 2)] + [r for r in range(count - 1, 0, -2)]
    place = [ring.index(r) for r in range(count)]
    right = [(ring[i], ring[(i + 1) % count]) for i in range(count)]
    left = [(b, a) for a, b in right]
    far = count // 2
    weight_b = weight.astype(jnp.bfloat16)
    all_targets = lax.all_gather(targets, "rep", axis=0, tiled=False)

    from_left = [[inputs[:half], inputs[half:]]]
    from_right = [[inputs[:half], inputs[half:]]]
    for step in range(1, far + 1):
        last = step == far
        a = lax.ppermute(from_left[-1][0], "rep", right)
        d = lax.ppermute(from_right[-1][1], "rep", left)
        b = None if last else lax.ppermute(from_left[-1][1], "rep", right)
        c = None if last else lax.ppermute(from_right[-1][0], "rep", left)
        from_left.append([a, b])
        from_right.append([c, d])
    phases = [[(0, from_left[0])]]
    for step in range(1, far):
        phases.append([(-step, from_left[step]), (step, from_right[step])])
    phases.append([(far, [from_left[far][0], from_right[far][1]])])
    ring_ids = jnp.array(ring, jnp.int32)
    my_place = jnp.array(place, jnp.int32)[rep]
    offsets = [offset for phase in phases for offset, _ in phase]
    ids = ring_ids[(my_place + jnp.array(offsets, jnp.int32)) % count]

    table_columns = lax.dynamic_slice(table, (0, rep * columns), (table.shape[0], columns))
    ordered = all_targets[ids]
    choice = (ordered[:, :, None] == jnp.arange(table.shape[0], dtype=jnp.int32)).astype(jnp.bfloat16)
    wanted = jnp.dot(
        choice.reshape(count * quarter, table.shape[0]), table_columns, preferred_element_type=jnp.float32
    ).reshape(count, quarter, columns)

    core_bit = shard & 1
    y_bit = shard >> 1
    swap_core = [(i, i ^ 1) for i in range(4)]
    swap_y = [(i, i ^ 2) for i in range(4)]
    grads = []
    sums = []
    pairs = []
    at = 0
    for phase in phases:
        xs = [x for _, chunk in phase for x in chunk]
        news = len(phase)
        partial = jnp.concatenate(
            [jnp.dot(x, weight_b, preferred_element_type=jnp.float32) for x in xs]
        ).reshape(news, 2, 2, quarter, columns)
        keep = jnp.where(core_bit == 1, partial[:, :, 1], partial[:, :, 0])
        send = jnp.where(core_bit == 1, partial[:, :, 0], partial[:, :, 1])
        keep = keep + lax.ppermute(send, "shard", swap_core)
        send = jnp.where(y_bit == 1, keep[:, 0], keep[:, 1])
        keep = jnp.where(y_bit == 1, keep[:, 1], keep[:, 0])
        outputs = keep + lax.ppermute(send, "shard", swap_y)
        error = ((outputs - wanted[at : at + news]) / rows).astype(jnp.bfloat16)
        other = lax.ppermute(error, "shard", swap_y)
        pair = jnp.stack(
            [jnp.where(y_bit == 1, other, error), jnp.where(y_bit == 1, error, other)], axis=1
        )
        other = lax.ppermute(pair, "shard", swap_core)
        errors = jnp.stack(
            [jnp.where(core_bit == 1, other, pair), jnp.where(core_bit == 1, pair, other)], axis=2
        ).reshape(news, rows, columns)
        pairs += [(i, at + n) for n in range(news) for i in range(at + n + 1)]
        made, part = grad_step(xs, 2, errors, grads)
        grads = grads + list(made)
        sums.append(part)
        at += news

    smem = pl.BlockSpec(memory_space=pltpu.SMEM)
    products = pl.pallas_call(
        functools.partial(place_kernel, pairs=pairs),
        in_specs=[smem] + [pl.BlockSpec(memory_space=pltpu.VMEM)] * len(sums),
        out_shape=jax.ShapeDtypeStruct((8, 128), jnp.float32),
        compiler_params=pltpu.CompilerParams(vmem_limit_bytes=2 * 2**20),
        name="place",
    )(ids, *sums)
    products = products + lax.ppermute(products, "shard", swap_core)
    products = products + lax.ppermute(products, "shard", swap_y)
    bit = 1
    while bit < count:
        products = products + lax.ppermute(products, "rep", [(i, i ^ bit) for i in range(count)])
        bit *= 2
    tile = 256
    block = pl.BlockSpec((tile, columns), lambda i: (i, 0))
    return pl.pallas_call(
        functools.partial(combine_kernel, count=count, tile=tile),
        grid=(features // tile,),
        in_specs=[smem, smem] + [block] * (1 + count),
        out_specs=[block, block],
        out_shape=[jax.ShapeDtypeStruct((features, columns), jnp.float32)] * 2,
        compiler_params=pltpu.CompilerParams(
            dimension_semantics=("arbitrary",), vmem_limit_bytes=16 * 2**20
        ),
        name="combine",
    )(ids, products, weight, *grads)


def gather_path(inputs, weight, table, targets):
    count = lax.axis_size("rep")
    rows = inputs.shape[0]
    features, columns = weight.shape
    rep = lax.axis_index("rep")
    all_inputs = lax.all_gather(inputs, "rep", axis=0, tiled=True)
    all_targets = lax.all_gather(targets, "rep", axis=0, tiled=False)
    partial = jnp.dot(all_inputs, weight.astype(jnp.bfloat16), preferred_element_type=jnp.float32)
    outputs = lax.psum_scatter(
        partial.reshape(count, rows, columns), "shard", scatter_dimension=1, tiled=True
    )
    table_columns = lax.dynamic_slice(table, (0, rep * columns), (table.shape[0], columns))
    wanted = table_columns[all_targets].astype(jnp.float32)
    error = ((outputs - wanted) / rows).astype(jnp.bfloat16)
    errors = lax.all_gather(error, "shard", axis=1, tiled=True)
    grads = lax.dot_general(
        all_inputs.reshape(count, rows, features),
        errors,
        (((1,), (1,)), ((0,), (0,))),
        preferred_element_type=jnp.float32,
    )
    products = lax.dot_general(
        grads, grads, (((1, 2), (1, 2)), ((), ())), precision=lax.Precision.HIGHEST
    )
    products = lax.psum(products, ("rep", "shard"))
    weights = jnp.stack(tree_weights(lambda a, b: products[a, b], count))
    combined = jnp.sum(weights[:, None, None] * grads, axis=0)
    return combined, weight - step_size * combined


def on_device(inputs, weight, table, targets):
    count = lax.axis_size("rep")
    fits = lax.axis_size("shard") == 4 and count in (4, 8)
    fits = fits and inputs.shape[0] % 64 == 0 and weight.shape[0] % 256 == 0 and weight.shape[1] % 128 == 0
    if fits:
        return tuple(ring_path(inputs, weight, table, targets))
    return gather_path(inputs, weight, table, targets)


def solution(mesh):
    in_specs = (P("rep", "shard"), P("shard", "rep"), P(), P(("rep", "shard")))
    out_specs = (P("shard", "rep"), P("shard", "rep"))
    return jax.shard_map(
        on_device, mesh=mesh, in_specs=in_specs, out_specs=out_specs, check_vma=False
    )
```

```python
import functools

import jax
import jax.numpy as jnp
from jax import lax
from jax.experimental import pallas as pl
from jax.experimental.pallas import tpu as pltpu
from jax.sharding import PartitionSpec as P


epsilon = 1e-06
step_size = 0.05


def mix_pair(cross, norm_low, norm_high):
    norm_low = jnp.maximum(norm_low, 0.0)
    norm_high = jnp.maximum(norm_high, 0.0)
    bound = jnp.sqrt(norm_low) * jnp.sqrt(norm_high)
    cross = jnp.minimum(jnp.maximum(cross, -bound), bound)
    return (
        1.0 - cross / (2.0 * (norm_low + epsilon)),
        1.0 - cross / (2.0 * (norm_high + epsilon)),
    )


def tree_weights(entry, count):
    products = {(a, b): entry(a, b) for a in range(count) for b in range(a, count)}
    weights = [None] * count
    group = 1
    alive = count
    while alive > 1:
        factors = []
        for m in range(alive // 2):
            low, high = mix_pair(
                products[2 * m, 2 * m + 1], products[2 * m, 2 * m], products[2 * m + 1, 2 * m + 1]
            )
            factors.append((low, high))
            for r in range(2 * m * group, (2 * m + 1) * group):
                weights[r] = low if weights[r] is None else weights[r] * low
            for r in range((2 * m + 1) * group, (2 * m + 2) * group):
                weights[r] = high if weights[r] is None else weights[r] * high
        merged = {}
        for a in range(alive // 2):
            for b in range(a, alive // 2):
                terms = [
                    factors[a][i]
                    * factors[b][j]
                    * products[min(2 * a + i, 2 * b + j), max(2 * a + i, 2 * b + j)]
                    for i in range(2)
                    for j in range(2)
                ]
                merged[a, b] = (terms[0] + terms[3]) + (terms[1] + terms[2])
        products = merged
        alive //= 2
        group *= 2
    return weights


def grad_kernel(where, *refs, news, olds):
    xs = refs[: 2 * news]
    own, other = refs[2 * news : 2 * news + 2]
    old = refs[2 * news + 2 : 2 * news + 2 + olds]
    new = refs[2 * news + 2 + olds : 2 * news + 2 + olds + news]
    sums = refs[-1]
    for n in range(news):
        new[n][...] = lax.dot_general(
            jnp.concatenate([xs[2 * n][...], xs[2 * n + 1][...]], axis=0),
            jnp.concatenate([own[n, 0], own[n, 1], other[n, 0], other[n, 1]], axis=0),
            (((0,), (0,)), ((), ())),
            preferred_element_type=jnp.float32,
        )
    every = list(old) + list(new)
    pairs = [(i, olds + n) for n in range(news) for i in range(olds + n + 1)]
    features, columns = new[0].shape

    def body(step, carry):
        carry = list(carry)
        for c in range(columns // 128):
            got = [ref[pl.ds(pl.multiple_of(step * 8, 8), 8), c * 128 : (c + 1) * 128] for ref in every]
            for k, (i, j) in enumerate(pairs):
                carry[k] = carry[k] + got[i] * got[j]
        return tuple(carry)

    totals = lax.fori_loop(
        0, features // 8, body, tuple(jnp.zeros((8, 128), jnp.float32) for _ in pairs), unroll=4
    )
    for k in range(len(pairs)):
        sums[k] = totals[k]


def ring_replica(index, count):
    return jnp.where(index < count // 2, 2 * index, 2 * (count - 1 - index) + 1)


def ring_place(replica, count):
    return jnp.where(replica % 2 == 0, replica // 2, count - 1 - replica // 2)


def replica_at(rep, offset, count):
    index = ring_place(rep, count) + offset % count
    return ring_replica(jnp.where(index >= count, index - count, index), count)


def place_kernel(where, *refs, pairs, offsets):
    out = refs[-1]
    count = len(offsets)
    ids = [replica_at(where[0], offset, count) for offset in offsets]
    row = lax.broadcasted_iota(jnp.int32, (8, 128), 0)
    column = lax.broadcasted_iota(jnp.int32, (8, 128), 1)
    tile = jnp.zeros((8, 128), jnp.float32)
    at = 0
    for ref in refs[:-1]:
        for k in range(ref.shape[0]):
            i, j = pairs[at]
            at += 1
            total = jnp.sum(ref[k], axis=(0, 1), keepdims=True)
            here = ((row == ids[i]) & (column == ids[j])) | ((row == ids[j]) & (column == ids[i]))
            tile = jnp.where(here, total, tile)
    out[...] = tile


def combine_kernel(where, products, weight, *refs, offsets, tile):
    count = len(offsets)
    grads = refs[:count]
    combined, new_weight, factors = refs[count:]

    @pl.when(pl.program_id(0) == 0)
    def _():
        weights = tree_weights(lambda a, b: jnp.full((8, 128), products[a, b], jnp.float32), count)
        for i, offset in enumerate(offsets):
            mine = replica_at(where[0], offset, count)
            value = weights[0]
            for a in range(1, count):
                value = jnp.where(mine == a, weights[a], value)
            factors[i] = value

    local = [factors[i] for i in range(count)]
    columns = combined.shape[1] // 128

    def body(step, carry):
        rows = pl.ds(pl.multiple_of(step * 8, 8), 8)
        for c in range(columns):
            lanes = slice(c * 128, (c + 1) * 128)
            total = local[0] * grads[0][rows, lanes]
            for i in range(1, count):
                total = total + local[i] * grads[i][rows, lanes]
            combined[rows, lanes] = total
            new_weight[rows, lanes] = weight[rows, lanes] - step_size * total
        return carry

    lax.fori_loop(0, tile // 8, body, 0, unroll=4)


def local_call(kernel, shapes, *args):
    vmem = pl.BlockSpec(memory_space=pltpu.VMEM)
    out = pl.pallas_call(
        kernel,
        in_specs=[pl.BlockSpec(memory_space=pltpu.SMEM)] + [vmem] * (len(args) - 1),
        out_specs=[vmem] * len(shapes),
        out_shape=[jax.ShapeDtypeStruct(shape, dtype) for shape, dtype in shapes],
        compiler_params=pltpu.CompilerParams(vmem_limit_bytes=12 * 2**20),
    )(*args)
    return out


def rows_kernel(where, inputs, mine, theirs):
    core = where[1] & 1
    quarter = mine.shape[0] // 2
    for y in range(2):
        for out, side in ((mine, core), (theirs, 1 - core)):
            start = pl.multiple_of((2 * y + side) * quarter, quarter)
            out[y * quarter : (y + 1) * quarter] = inputs[pl.ds(start, quarter)]


def cast_kernel(where, weight, weight_b):
    weight_b[...] = weight[...].astype(weight_b.dtype)


def outputs_kernel(where, *refs):
    news = (len(refs) - 4) // 2
    weight_b, weight_other, keep, send = refs[2 * news :]
    quarter = keep.shape[1]
    upper = where[1] >> 1 == 1
    for n in range(news):
        made = jnp.dot(refs[n][...], weight_b[...], preferred_element_type=jnp.float32)
        made += jnp.dot(refs[news + n][...], weight_other[...], preferred_element_type=jnp.float32)
        first, second = made[:quarter], made[quarter:]
        keep[n] = jnp.where(upper, second, first)
        send[n] = jnp.where(upper, first, second)


def error_kernel(where, mine, got, wanted, error, *, at, rows):
    for n in range(error.shape[0]):
        error[n] = ((mine[n] + got[n] - wanted[at + n]) / rows).astype(error.dtype)


def pair_kernel(where, mine, got, pair):
    upper = where[1] >> 1 == 1
    for n in range(pair.shape[0]):
        pair[n, 0] = jnp.where(upper, got[n], mine[n])
        pair[n, 1] = jnp.where(upper, mine[n], got[n])


def wanted_kernel(where, *refs, offsets):
    targets, table, wanted = refs
    count = len(offsets)
    candidates = lax.broadcasted_iota(jnp.int32, (table.shape[0], wanted.shape[1]), 0)
    for i, offset in enumerate(offsets):
        slot = replica_at(where[0], offset, count) ^ where[0]
        chosen = targets[0:1]
        for k in range(1, count):
            chosen = jnp.where(slot == k, targets[k : k + 1], chosen)
        hot = (candidates == chosen).astype(table.dtype)
        wanted[i] = lax.dot_general(
            hot, table[...], (((0,), (0,)), ((), ())), preferred_element_type=jnp.float32
        )


def ring_path(inputs, weight, table, targets):
    count = lax.axis_size("rep")
    rows = inputs.shape[0]
    features, columns = weight.shape
    quarter = rows // 4
    right = []
    left = []
    for i in range(count):
        ends = [2 * r if r < count // 2 else 2 * (count - 1 - r) + 1 for r in (i, (i + 1) % count)]
        right.append((ends[0], ends[1]))
        left.append((ends[1], ends[0]))
    far = count // 2
    where = jnp.stack([lax.axis_index("rep"), lax.axis_index("shard")])

    half = ((rows // 2, features), inputs.dtype)
    from_left = [local_call(rows_kernel, (half, half), where, inputs)]
    from_right = [from_left[0]]
    for step in range(1, far + 1):
        last = step == far
        a = lax.ppermute(from_left[-1][0], "rep", right)
        d = lax.ppermute(from_right[-1][1], "rep", left)
        b = None if last else lax.ppermute(from_left[-1][1], "rep", right)
        c = None if last else lax.ppermute(from_right[-1][0], "rep", left)
        from_left.append([a, b])
        from_right.append([c, d])
    phases = [[(0, from_left[0])]]
    for step in range(1, far):
        phases.append([(-step, from_left[step]), (step, from_right[step])])
    phases.append([(far, [from_left[far][0], from_right[far][1]])])
    offsets = tuple(offset for phase in phases for offset, _ in phase)

    all_targets = targets[None]
    for i in range(count.bit_length() - 1):
        pairs = [(r, r ^ 1 << i) for r in range(count)]
        all_targets = jnp.concatenate([all_targets, lax.ppermute(all_targets, "rep", pairs)])
    wanted = pl.pallas_call(
        functools.partial(wanted_kernel, offsets=offsets),
        grid_spec=pltpu.PrefetchScalarGridSpec(
            num_scalar_prefetch=1,
            grid=(1,),
            in_specs=[
                pl.BlockSpec((count, quarter), lambda i, where: (0, 0)),
                pl.BlockSpec((table.shape[0], columns), lambda i, where: (0, where[0])),
            ],
            out_specs=pl.BlockSpec((count, quarter, columns), lambda i, where: (0, 0, 0)),
        ),
        out_shape=jax.ShapeDtypeStruct((count, quarter, columns), jnp.float32),
        compiler_params=pltpu.CompilerParams(vmem_limit_bytes=8 * 2**20),
        name="wanted",
    )(where, all_targets, table)

    swap_core = [(i, i ^ 1) for i in range(4)]
    swap_y = [(i, i ^ 2) for i in range(4)]
    grads = []
    sums = []
    pairs = []
    at = 0
    (weight_b,) = local_call(cast_kernel, ((weight.shape, jnp.bfloat16),), where, weight)
    weight_other = lax.ppermute(weight_b, "shard", swap_core)
    for phase in phases:
        xs = [x for _, chunk in phase for x in chunk]
        news = len(phase)
        whole = ((news, 2, quarter, columns), jnp.bfloat16)
        part = ((news, quarter, columns), jnp.float32)
        others = [lax.ppermute(x, "shard", swap_core) for x in xs[1::2]]
        keep, send = local_call(
            outputs_kernel, (part, part), where, *xs[::2], *others, weight_b, weight_other
        )
        got = lax.ppermute(send, "shard", swap_y)
        (error,) = local_call(
            functools.partial(error_kernel, at=at, rows=rows),
            ((part[0], jnp.bfloat16),),
            where,
            keep,
            got,
            wanted,
        )
        got = lax.ppermute(error, "shard", swap_y)
        (own,) = local_call(pair_kernel, (whole,), where, error, got)
        other = lax.ppermute(own, "shard", swap_core)
        fresh = [(i, at + n) for n in range(news) for i in range(at + n + 1)]
        made = local_call(
            functools.partial(grad_kernel, news=news, olds=at),
            ((weight.shape, jnp.float32),) * news + (((len(fresh), 8, 128), jnp.float32),),
            where,
            *xs,
            own,
            other,
            *grads,
        )
        pairs += fresh
        grads = grads + list(made[:news])
        sums.append(made[news])
        at += news

    (products,) = local_call(
        functools.partial(place_kernel, pairs=pairs, offsets=offsets),
        (((8, 128), jnp.float32),),
        where,
        *sums,
    )
    products = products + lax.ppermute(products, "shard", swap_core)
    products = products + lax.ppermute(products, "shard", swap_y)
    bit = 1
    while bit < count:
        products = products + lax.ppermute(products, "rep", [(i, i ^ bit) for i in range(count)])
        bit *= 2
    tile = features // 4
    smem = pl.BlockSpec(memory_space=pltpu.SMEM)
    block = pl.BlockSpec((tile, columns), lambda i: (i, 0))
    return pl.pallas_call(
        functools.partial(combine_kernel, offsets=offsets, tile=tile),
        grid=(features // tile,),
        in_specs=[smem, smem] + [block] * (1 + count),
        out_specs=[block, block],
        out_shape=[jax.ShapeDtypeStruct((features, columns), jnp.float32)] * 2,
        scratch_shapes=[pltpu.VMEM((count, 8, 128), jnp.float32)],
        compiler_params=pltpu.CompilerParams(
            dimension_semantics=("arbitrary",), vmem_limit_bytes=16 * 2**20
        ),
        name="combine",
    )(where, products, weight, *grads)


def gather_path(inputs, weight, table, targets):
    count = lax.axis_size("rep")
    rows = inputs.shape[0]
    features, columns = weight.shape
    rep = lax.axis_index("rep")
    all_inputs = lax.all_gather(inputs, "rep", axis=0, tiled=True)
    all_targets = lax.all_gather(targets, "rep", axis=0, tiled=False)
    partial = jnp.dot(all_inputs, weight.astype(jnp.bfloat16), preferred_element_type=jnp.float32)
    outputs = lax.psum_scatter(
        partial.reshape(count, rows, columns), "shard", scatter_dimension=1, tiled=True
    )
    table_columns = lax.dynamic_slice(table, (0, rep * columns), (table.shape[0], columns))
    wanted = table_columns[all_targets].astype(jnp.float32)
    error = ((outputs - wanted) / rows).astype(jnp.bfloat16)
    errors = lax.all_gather(error, "shard", axis=1, tiled=True)
    grads = lax.dot_general(
        all_inputs.reshape(count, rows, features),
        errors,
        (((1,), (1,)), ((0,), (0,))),
        preferred_element_type=jnp.float32,
    )
    products = lax.dot_general(
        grads, grads, (((1, 2), (1, 2)), ((), ())), precision=lax.Precision.HIGHEST
    )
    products = lax.psum(products, ("rep", "shard"))
    weights = jnp.stack(tree_weights(lambda a, b: products[a, b], count))
    combined = jnp.sum(weights[:, None, None] * grads, axis=0)
    return combined, weight - step_size * combined


def solution(mesh):
    count, shards = mesh.shape["rep"], mesh.shape["shard"]
    ring = shards == 4 and count in (4, 8)

    def on_device(inputs, weight, table, targets):
        if ring:
            return tuple(ring_path(inputs, weight, table, targets))
        return gather_path(inputs, weight, table, targets)

    in_specs = (P("rep", "shard"), P("shard", "rep"), P(), P(("rep", "shard")))
    out_specs = (P("shard", "rep"), P("shard", "rep"))
    return jax.shard_map(
        on_device, mesh=mesh, in_specs=in_specs, out_specs=out_specs, check_vma=False
    )
```

```python
import functools

import jax
import jax.numpy as jnp
from jax import lax
from jax.experimental import pallas as pl
from jax.experimental.pallas import tpu as pltpu
from jax.sharding import PartitionSpec as P


epsilon = 1e-06
step_size = 0.05


def mix_pair(cross, norm_low, norm_high):
    norm_low = jnp.maximum(norm_low, 0.0)
    norm_high = jnp.maximum(norm_high, 0.0)
    bound = jnp.sqrt(norm_low) * jnp.sqrt(norm_high)
    cross = jnp.minimum(jnp.maximum(cross, -bound), bound)
    return (
        1.0 - cross / (2.0 * (norm_low + epsilon)),
        1.0 - cross / (2.0 * (norm_high + epsilon)),
    )


def tree_weights(entry, count):
    products = {(a, b): entry(a, b) for a in range(count) for b in range(a, count)}
    weights = [None] * count
    group = 1
    alive = count
    while alive > 1:
        factors = []
        for m in range(alive // 2):
            low, high = mix_pair(
                products[2 * m, 2 * m + 1], products[2 * m, 2 * m], products[2 * m + 1, 2 * m + 1]
            )
            factors.append((low, high))
            for r in range(2 * m * group, (2 * m + 1) * group):
                weights[r] = low if weights[r] is None else weights[r] * low
            for r in range((2 * m + 1) * group, (2 * m + 2) * group):
                weights[r] = high if weights[r] is None else weights[r] * high
        merged = {}
        for a in range(alive // 2):
            for b in range(a, alive // 2):
                terms = [
                    factors[a][i]
                    * factors[b][j]
                    * products[min(2 * a + i, 2 * b + j), max(2 * a + i, 2 * b + j)]
                    for i in range(2)
                    for j in range(2)
                ]
                merged[a, b] = (terms[0] + terms[3]) + (terms[1] + terms[2])
        products = merged
        alive //= 2
        group *= 2
    return weights


def grad_kernel(where, *refs, blocks, phases, olds):
    news = len(blocks)
    xs = refs[: 2 * news]
    errors = refs[2 * news : 2 * news + 4 * phases]
    old = refs[2 * news + 4 * phases : 2 * news + 4 * phases + olds]
    new = refs[2 * news + 4 * phases + olds : 3 * news + 4 * phases + olds]
    sums = refs[-1]
    second = where[1] & 1 == 1
    upper = where[1] >> 1 == 1
    for n, ends in enumerate(blocks):
        parts = []
        for half, (phase, slot) in enumerate(ends):
            mine, across, other, other_across = [ref[slot] for ref in errors[4 * phase : 4 * phase + 4]]
            if half:
                here, there = jnp.where(upper, mine, across), jnp.where(upper, other, other_across)
            else:
                here, there = jnp.where(upper, across, mine), jnp.where(upper, other_across, other)
            parts += [jnp.where(second, there, here), jnp.where(second, here, there)]
        new[n][...] = lax.dot_general(
            jnp.concatenate([xs[2 * n][...], xs[2 * n + 1][...]], axis=0),
            jnp.concatenate(parts, axis=0),
            (((0,), (0,)), ((), ())),
            preferred_element_type=jnp.float32,
        )
    every = list(old) + list(new)
    pairs = [(i, olds + n) for n in range(news) for i in range(olds + n + 1)]
    features, columns = new[0].shape

    def body(step, carry):
        carry = list(carry)
        for c in range(columns // 128):
            got = [ref[pl.ds(pl.multiple_of(step * 8, 8), 8), c * 128 : (c + 1) * 128] for ref in every]
            for k, (i, j) in enumerate(pairs):
                carry[k] = carry[k] + got[i] * got[j]
        return tuple(carry)

    totals = lax.fori_loop(
        0, features // 8, body, tuple(jnp.zeros((8, 128), jnp.float32) for _ in pairs), unroll=4
    )
    for k in range(len(pairs)):
        sums[k] = totals[k]


def ring_replica(index, count):
    return jnp.where(index < count // 2, 2 * index, 2 * (count - 1 - index) + 1)


def ring_place(replica, count):
    return jnp.where(replica % 2 == 0, replica // 2, count - 1 - replica // 2)


def replica_at(rep, offset, count):
    index = ring_place(rep, count) + offset % count
    return ring_replica(jnp.where(index >= count, index - count, index), count)


def place_kernel(where, *refs, pairs, offsets):
    out = refs[-1]
    count = len(offsets)
    ids = [replica_at(where[0], offset, count) for offset in offsets]
    row = lax.broadcasted_iota(jnp.int32, (8, 128), 0)
    column = lax.broadcasted_iota(jnp.int32, (8, 128), 1)
    tile = jnp.zeros((8, 128), jnp.float32)
    at = 0
    for ref in refs[:-1]:
        for k in range(ref.shape[0]):
            i, j = pairs[at]
            at += 1
            total = jnp.sum(ref[k], axis=(0, 1), keepdims=True)
            here = ((row == ids[i]) & (column == ids[j])) | ((row == ids[j]) & (column == ids[i]))
            tile = jnp.where(here, total, tile)
    out[...] = tile


def combine_kernel(where, products, weight, *refs, offsets, parts):
    count = len(offsets)
    grads = refs[:count]
    combined, new_weight, made, moved, sems = refs[count:]
    weights = tree_weights(lambda a, b: jnp.full((8, 128), products[a, b], jnp.float32), count)
    local = []
    for offset in offsets:
        mine = replica_at(where[0], offset, count)
        value = weights[0]
        for a in range(1, count):
            value = jnp.where(mine == a, weights[a], value)
        local.append(value)
    features, columns = made.shape
    tile = features // parts

    def copies(part):
        rows = pl.ds(part * tile, tile)
        return (
            pltpu.make_async_copy(made.at[rows], combined.at[rows], sems.at[0, part]),
            pltpu.make_async_copy(moved.at[rows], new_weight.at[rows], sems.at[1, part]),
        )

    for part in range(parts):

        def body(step, carry):
            rows = pl.ds(pl.multiple_of(part * tile + step * 8, 8), 8)
            for c in range(columns // 128):
                lanes = slice(c * 128, (c + 1) * 128)
                total = local[0] * grads[0][rows, lanes]
                for i in range(1, count):
                    total = total + local[i] * grads[i][rows, lanes]
                made[rows, lanes] = total
                moved[rows, lanes] = weight[rows, lanes] - step_size * total
            return carry

        lax.fori_loop(0, tile // 8, body, 0, unroll=4)
        for copy in copies(part):
            copy.start()
    for part in range(parts):
        for copy in copies(part):
            copy.wait()


def local_call(kernel, shapes, *args):
    vmem = pl.BlockSpec(memory_space=pltpu.VMEM)
    out = pl.pallas_call(
        kernel,
        in_specs=[pl.BlockSpec(memory_space=pltpu.SMEM)] + [vmem] * (len(args) - 1),
        out_specs=[vmem] * len(shapes),
        out_shape=[jax.ShapeDtypeStruct(shape, dtype) for shape, dtype in shapes],
        compiler_params=pltpu.CompilerParams(vmem_limit_bytes=12 * 2**20),
    )(*args)
    return out


def cast_kernel(where, weight, weight_b):
    weight_b[...] = weight[...].astype(weight_b.dtype)


def rows_of(core, quarter):
    return pl.ds(pl.multiple_of(core * quarter, quarter), quarter)


def pick_kernel(where, *refs):
    out = refs[-1]
    theirs = rows_of(1 - (where[1] & 1), out.shape[1])
    for n in range(out.shape[0]):
        out[n] = refs[n][theirs]


def join_kernel(where, *refs):
    refs[-1][...] = jnp.concatenate([ref[...] for ref in refs[:-1]])


def outputs_kernel(where, *refs):
    weight_b, weight_other, keep, send = refs[-4:]
    slots, quarter = keep.shape[:2]
    xs = refs[: 2 * slots]
    got = refs[2 * slots : -4]
    upper = where[1] >> 1 == 1
    rows = rows_of(where[1] & 1, quarter)
    for n in range(slots):
        mine = jnp.concatenate([xs[2 * n + half][rows] for half in range(2)])
        if len(got) == 1:
            other = jnp.concatenate([got[0][2 * n + half] for half in range(2)])
        else:
            other = jnp.concatenate([got[2 * n + half][rows] for half in range(2)])
        made = jnp.dot(mine, weight_b[...], preferred_element_type=jnp.float32)
        made += jnp.dot(other, weight_other[...], preferred_element_type=jnp.float32)
        first, second = made[:quarter], made[quarter:]
        keep[n] = jnp.where(upper, second, first)
        send[n] = jnp.where(upper, first, second)


def error_kernel(where, *refs, at, rows):
    wanted, error = refs[-2:]
    n = 0
    for mine, got in zip(refs[:-2:2], refs[1:-2:2]):
        for slot in range(mine.shape[0]):
            error[n] = ((mine[slot] + got[slot] - wanted[at + n]) / rows).astype(error.dtype)
            n += 1


def wanted_kernel(where, *refs, slots):
    table, wanted = refs[-2:]
    count = len(slots)
    targets = [ref[k : k + 1] for ref in refs[:-2] for k in range(ref.shape[0])]
    candidates = lax.broadcasted_iota(jnp.int32, (table.shape[0], wanted.shape[1]), 0)
    for i, (first, second) in enumerate(slots):
        offset = jnp.where(where[1] >> 1 == 1, second % count, first % count)
        place = replica_at(where[0], offset, count) ^ where[0]
        chosen = targets[0]
        for k in range(1, count):
            chosen = jnp.where(place == k, targets[k], chosen)
        hot = (candidates == chosen).astype(table.dtype)
        wanted[i] = lax.dot_general(
            hot, table[...], (((0,), (0,)), ((), ())), preferred_element_type=jnp.float32
        )


def ring_path(inputs, weight, table, targets):
    count = lax.axis_size("rep")
    rows = inputs.shape[0]
    features, columns = weight.shape
    quarter = rows // 4
    right = []
    left = []
    for i in range(count):
        ends = [2 * r if r < count // 2 else 2 * (count - 1 - r) + 1 for r in (i, (i + 1) % count)]
        right.append((ends[0], ends[1]))
        left.append((ends[1], ends[0]))
    far = count // 2
    where = jnp.stack([lax.axis_index("rep"), lax.axis_index("shard")])

    from_left = [[inputs[: rows // 2], inputs[rows // 2 :]]]
    from_right = [from_left[0]]
    for step in range(1, far + 1):
        last = step == far
        a = lax.ppermute(from_left[-1][0], "rep", right)
        d = lax.ppermute(from_right[-1][1], "rep", left)
        b = None if last else lax.ppermute(from_left[-1][1], "rep", right)
        c = None if last else lax.ppermute(from_right[-1][0], "rep", left)
        from_left.append([a, b])
        from_right.append([c, d])
    halves = {0: from_left[0], far: [from_left[far][0], from_right[far][1]]}
    for step in range(1, far):
        halves[-step] = from_left[step]
        halves[step] = from_right[step]
    phases = [[(0, 0)]]
    phases += [[(-step, step), (step, -step)] for step in range(1, far - 1)]
    phases += [[(1 - far, far - 1)], [(far - 1, 1 - far)], [(far, far)]]
    slots = tuple(slot for phase in phases for slot in phase)
    joined = [[0, 1]] + [[m] for m in range(2, far - 1)] + [[far - 1, far], [far + 1]]
    groups = [[0, -1, 1]] + [[-step, step] for step in range(2, far)] + [[far]]
    offsets = tuple(offset for group in groups for offset in group)

    pieces = [targets[None]]
    for i in range(count.bit_length() - 1):
        block = pieces[0]
        if i:
            shape = ((1 << i, quarter), targets.dtype)
            (block,) = local_call(join_kernel, (shape,), where, *pieces)
        pieces.append(lax.ppermute(block, "rep", [(r, r ^ 1 << i) for r in range(count)]))
    wanted = pl.pallas_call(
        functools.partial(wanted_kernel, slots=slots),
        grid_spec=pltpu.PrefetchScalarGridSpec(
            num_scalar_prefetch=1,
            grid=(1,),
            in_specs=[pl.BlockSpec(piece.shape, lambda i, where: (0, 0)) for piece in pieces]
            + [pl.BlockSpec((table.shape[0], columns), lambda i, where: (0, where[0]))],
            out_specs=pl.BlockSpec((count, quarter, columns), lambda i, where: (0, 0, 0)),
        ),
        out_shape=jax.ShapeDtypeStruct((count, quarter, columns), jnp.float32),
        compiler_params=pltpu.CompilerParams(vmem_limit_bytes=8 * 2**20),
        name="wanted",
    )(where, *pieces, table)

    swap_core = [(i, i ^ 1) for i in range(4)]
    swap_y = [(i, i ^ 2) for i in range(4)]
    (weight_b,) = local_call(cast_kernel, ((weight.shape, jnp.bfloat16),), where, weight)
    weight_other = lax.ppermute(weight_b, "shard", swap_core)
    summed = []
    for phase in phases:
        part = ((len(phase), quarter, columns), jnp.float32)
        xs = [halves[slot[half]][half] for slot in phase for half in range(2)]
        outgoing = xs
        if len(phase) > 1:
            shape = ((len(xs), quarter, features), inputs.dtype)
            outgoing = local_call(pick_kernel, (shape,), where, *xs)
        others = [lax.ppermute(x, "shard", swap_core) for x in outgoing]
        keep, send = local_call(outputs_kernel, (part, part), where, *xs, *others, weight_b, weight_other)
        summed += [(keep, lax.ppermute(send, "shard", swap_y))]

    errors = []
    errors_at = {}
    at = 0
    for m, members in enumerate(joined):
        mine = [slot for phase in members for slot in phases[phase]]
        for n, ends in enumerate(mine):
            errors_at[ends[0], 0] = (m, n)
            errors_at[ends[1], 1] = (m, n)
        (error,) = local_call(
            functools.partial(error_kernel, at=at, rows=rows),
            (((len(mine), quarter, columns), jnp.bfloat16),),
            where,
            *[part for phase in members for part in summed[phase]],
            wanted,
        )
        across = lax.ppermute(error, "shard", swap_y)
        other = lax.ppermute(error, "shard", swap_core)
        errors.append((error, across, other, lax.ppermute(across, "shard", swap_core)))
        at += len(mine)

    grads = []
    sums = []
    pairs = []
    for group in groups:
        olds = len(grads)
        needed = sorted({errors_at[offset, half][0] for offset in group for half in range(2)})
        blocks = tuple(
            tuple((needed.index(errors_at[offset, half][0]), errors_at[offset, half][1]) for half in range(2))
            for offset in group
        )
        fresh = [(i, olds + n) for n in range(len(group)) for i in range(olds + n + 1)]
        made = local_call(
            functools.partial(grad_kernel, blocks=blocks, phases=len(needed), olds=olds),
            ((weight.shape, jnp.float32),) * len(group) + (((len(fresh), 8, 128), jnp.float32),),
            where,
            *[halves[offset][half] for offset in group for half in range(2)],
            *[part for phase in needed for part in errors[phase]],
            *grads,
        )
        pairs += fresh
        grads = grads + list(made[: len(group)])
        sums.append(made[len(group)])

    (products,) = local_call(
        functools.partial(place_kernel, pairs=pairs, offsets=offsets), (((8, 128), jnp.float32),), where, *sums
    )
    products = products + lax.ppermute(products, "shard", swap_core)
    products = products + lax.ppermute(products, "shard", swap_y)
    bit = 1
    while bit < count:
        products = products + lax.ppermute(products, "rep", [(i, i ^ bit) for i in range(count)])
        bit *= 2
    parts = 8
    smem = pl.BlockSpec(memory_space=pltpu.SMEM)
    vmem = pl.BlockSpec(memory_space=pltpu.VMEM)
    block = jax.ShapeDtypeStruct((features, columns), jnp.float32)
    return pl.pallas_call(
        functools.partial(combine_kernel, offsets=offsets, parts=parts),
        in_specs=[smem, smem] + [vmem] * (1 + count),
        out_specs=[pl.BlockSpec(memory_space=pltpu.HBM)] * 2,
        out_shape=[block] * 2,
        scratch_shapes=[pltpu.VMEM(block.shape, block.dtype)] * 2 + [pltpu.SemaphoreType.DMA((2, parts))],
        compiler_params=pltpu.CompilerParams(vmem_limit_bytes=12 * 2**20),
        name="combine",
    )(where, products, weight, *grads)


def gather_path(inputs, weight, table, targets):
    count = lax.axis_size("rep")
    rows = inputs.shape[0]
    features, columns = weight.shape
    rep = lax.axis_index("rep")
    all_inputs = lax.all_gather(inputs, "rep", axis=0, tiled=True)
    all_targets = lax.all_gather(targets, "rep", axis=0, tiled=False)
    partial = jnp.dot(all_inputs, weight.astype(jnp.bfloat16), preferred_element_type=jnp.float32)
    outputs = lax.psum_scatter(
        partial.reshape(count, rows, columns), "shard", scatter_dimension=1, tiled=True
    )
    table_columns = lax.dynamic_slice(table, (0, rep * columns), (table.shape[0], columns))
    wanted = table_columns[all_targets].astype(jnp.float32)
    error = ((outputs - wanted) / rows).astype(jnp.bfloat16)
    errors = lax.all_gather(error, "shard", axis=1, tiled=True)
    grads = lax.dot_general(
        all_inputs.reshape(count, rows, features),
        errors,
        (((1,), (1,)), ((0,), (0,))),
        preferred_element_type=jnp.float32,
    )
    products = lax.dot_general(
        grads, grads, (((1, 2), (1, 2)), ((), ())), precision=lax.Precision.HIGHEST
    )
    products = lax.psum(products, ("rep", "shard"))
    weights = jnp.stack(tree_weights(lambda a, b: products[a, b], count))
    combined = jnp.sum(weights[:, None, None] * grads, axis=0)
    return combined, weight - step_size * combined


def solution(mesh):
    count, shards = mesh.shape["rep"], mesh.shape["shard"]
    ring = shards == 4 and count == 8

    def on_device(inputs, weight, table, targets):
        if ring:
            return tuple(ring_path(inputs, weight, table, targets))
        return gather_path(inputs, weight, table, targets)

    in_specs = (P("rep", "shard"), P("shard", "rep"), P(), P(("rep", "shard")))
    out_specs = (P("shard", "rep"), P("shard", "rep"))
    return jax.shard_map(
        on_device, mesh=mesh, in_specs=in_specs, out_specs=out_specs, check_vma=False
    )
```

```python
import functools

import jax
import jax.numpy as jnp
from jax import lax
from jax.experimental import pallas as pl
from jax.experimental.pallas import tpu as pltpu
from jax.sharding import PartitionSpec as P


epsilon = 1e-06
step_size = 0.05


def mix_pair(cross, norm_low, norm_high):
    norm_low = jnp.maximum(norm_low, 0.0)
    norm_high = jnp.maximum(norm_high, 0.0)
    bound = jnp.sqrt(norm_low) * jnp.sqrt(norm_high)
    cross = jnp.minimum(jnp.maximum(cross, -bound), bound)
    return (
        1.0 - cross / (2.0 * (norm_low + epsilon)),
        1.0 - cross / (2.0 * (norm_high + epsilon)),
    )


def tree_weights(entry, count):
    products = {(a, b): entry(a, b) for a in range(count) for b in range(a, count)}
    weights = [None] * count
    group = 1
    alive = count
    while alive > 1:
        factors = []
        for m in range(alive // 2):
            low, high = mix_pair(
                products[2 * m, 2 * m + 1], products[2 * m, 2 * m], products[2 * m + 1, 2 * m + 1]
            )
            factors.append((low, high))
            for r in range(2 * m * group, (2 * m + 1) * group):
                weights[r] = low if weights[r] is None else weights[r] * low
            for r in range((2 * m + 1) * group, (2 * m + 2) * group):
                weights[r] = high if weights[r] is None else weights[r] * high
        merged = {}
        for a in range(alive // 2):
            for b in range(a, alive // 2):
                terms = [
                    factors[a][i]
                    * factors[b][j]
                    * products[min(2 * a + i, 2 * b + j), max(2 * a + i, 2 * b + j)]
                    for i in range(2)
                    for j in range(2)
                ]
                merged[a, b] = (terms[0] + terms[3]) + (terms[1] + terms[2])
        products = merged
        alive //= 2
        group *= 2
    return weights


def grad_kernel(where, *refs, blocks, phases, olds, pairs_of=None, offsets=None):
    news = len(blocks)
    xs = refs[: 2 * news]
    errors = refs[2 * news : 2 * news + 4 * phases]
    old = refs[2 * news + 4 * phases : 2 * news + 4 * phases + olds]
    rest = refs[2 * news + 4 * phases + olds :]
    done = rest[: -news - 1]
    new = rest[-news - 1 : -1]
    sums = rest[-1]
    second = where[1] & 1 == 1
    upper = where[1] >> 1 == 1
    for n, ends in enumerate(blocks):
        parts = []
        for half, (phase, slot) in enumerate(ends):
            mine, across, other, other_across = [ref[slot] for ref in errors[4 * phase : 4 * phase + 4]]
            if half:
                here, there = jnp.where(upper, mine, across), jnp.where(upper, other, other_across)
            else:
                here, there = jnp.where(upper, across, mine), jnp.where(upper, other_across, other)
            parts += [jnp.where(second, there, here), jnp.where(second, here, there)]
        new[n][...] = lax.dot_general(
            jnp.concatenate([xs[2 * n][...], xs[2 * n + 1][...]], axis=0),
            jnp.concatenate(parts, axis=0),
            (((0,), (0,)), ((), ())),
            preferred_element_type=jnp.float32,
        )
    every = list(old) + list(new)
    pairs = [(i, olds + n) for n in range(news) for i in range(olds + n + 1)]
    features, columns = new[0].shape

    def body(step, carry):
        carry = list(carry)
        for c in range(columns // 128):
            got = [ref[pl.ds(pl.multiple_of(step * 8, 8), 8), c * 128 : (c + 1) * 128] for ref in every]
            for k, (i, j) in enumerate(pairs):
                carry[k] = carry[k] + got[i] * got[j]
        return tuple(carry)

    totals = lax.fori_loop(
        0, features // 8, body, tuple(jnp.zeros((8, 128), jnp.float32) for _ in pairs), unroll=4
    )
    if offsets is None:
        for k in range(len(pairs)):
            sums[k] = totals[k]
    else:
        parts = [ref[k] for ref in done for k in range(ref.shape[0])] + list(totals)
        sums[...] = placed(where, parts, pairs_of, offsets)


def ring_replica(index, count):
    return jnp.where(index < count // 2, 2 * index, 2 * (count - 1 - index) + 1)


def ring_place(replica, count):
    return jnp.where(replica % 2 == 0, replica // 2, count - 1 - replica // 2)


def replica_at(rep, offset, count):
    index = ring_place(rep, count) + offset % count
    return ring_replica(jnp.where(index >= count, index - count, index), count)


def placed(where, parts, pairs, offsets):
    ids = [replica_at(where[0], offset, len(offsets)) for offset in offsets]
    row = lax.broadcasted_iota(jnp.int32, (8, 128), 0)
    column = lax.broadcasted_iota(jnp.int32, (8, 128), 1)
    tile = jnp.zeros((8, 128), jnp.float32)
    for part, (i, j) in zip(parts, pairs):
        total = jnp.sum(part, axis=(0, 1), keepdims=True)
        here = ((row == ids[i]) & (column == ids[j])) | ((row == ids[j]) & (column == ids[i]))
        tile = jnp.where(here, total, tile)
    return tile


def combine_kernel(where, products, weight, *refs, offsets, parts):
    count = len(offsets)
    grads = refs[:count]
    combined, new_weight, made, moved, sems = refs[count:]
    weights = tree_weights(lambda a, b: jnp.full((8, 128), products[a, b], jnp.float32), count)
    local = []
    for offset in offsets:
        mine = replica_at(where[0], offset, count)
        value = weights[0]
        for a in range(1, count):
            value = jnp.where(mine == a, weights[a], value)
        local.append(value)
    features, columns = made.shape
    tile = features // parts

    def copies(part):
        rows = pl.ds(part * tile, tile)
        return (
            pltpu.make_async_copy(made.at[rows], combined.at[rows], sems.at[0, part]),
            pltpu.make_async_copy(moved.at[rows], new_weight.at[rows], sems.at[1, part]),
        )

    for part in range(parts):

        def body(step, carry):
            rows = pl.ds(pl.multiple_of(part * tile + step * 8, 8), 8)
            for c in range(columns // 128):
                lanes = slice(c * 128, (c + 1) * 128)
                total = local[0] * grads[0][rows, lanes]
                for i in range(1, count):
                    total = total + local[i] * grads[i][rows, lanes]
                made[rows, lanes] = total
                moved[rows, lanes] = weight[rows, lanes] - step_size * total
            return carry

        lax.fori_loop(0, tile // 8, body, 0, unroll=4)
        for copy in copies(part):
            copy.start()
    for part in range(parts):
        for copy in copies(part):
            copy.wait()


def local_call(kernel, shapes, *args):
    vmem = pl.BlockSpec(memory_space=pltpu.VMEM)
    out = pl.pallas_call(
        kernel,
        in_specs=[pl.BlockSpec(memory_space=pltpu.SMEM)] + [vmem] * (len(args) - 1),
        out_specs=[vmem] * len(shapes),
        out_shape=[jax.ShapeDtypeStruct(shape, dtype) for shape, dtype in shapes],
        compiler_params=pltpu.CompilerParams(vmem_limit_bytes=12 * 2**20),
    )(*args)
    return out


def cast_kernel(where, weight, weight_b):
    weight_b[...] = weight[...].astype(weight_b.dtype)


def rows_of(core, quarter):
    return pl.ds(pl.multiple_of(core * quarter, quarter), quarter)


def pick_kernel(where, *refs):
    out = refs[-1]
    theirs = rows_of(1 - (where[1] & 1), out.shape[1])
    for n in range(out.shape[0]):
        out[n] = refs[n][theirs]


def join_kernel(where, *refs):
    refs[-1][...] = jnp.concatenate([ref[...] for ref in refs[:-1]])


def outputs_kernel(where, *refs):
    weight_b, weight_other, keep, send = refs[-4:]
    slots, quarter = keep.shape[:2]
    xs = refs[: 2 * slots]
    got = refs[2 * slots : -4]
    upper = where[1] >> 1 == 1
    rows = rows_of(where[1] & 1, quarter)
    for n in range(slots):
        mine = jnp.concatenate([xs[2 * n + half][rows] for half in range(2)])
        if len(got) == 1:
            other = jnp.concatenate([got[0][2 * n + half] for half in range(2)])
        else:
            other = jnp.concatenate([got[2 * n + half][rows] for half in range(2)])
        made = jnp.dot(mine, weight_b[...], preferred_element_type=jnp.float32)
        made += jnp.dot(other, weight_other[...], preferred_element_type=jnp.float32)
        first, second = made[:quarter], made[quarter:]
        keep[n] = jnp.where(upper, second, first)
        send[n] = jnp.where(upper, first, second)


def error_kernel(where, *refs, at, rows):
    wanted, error = refs[-2:]
    n = 0
    for mine, got in zip(refs[:-2:2], refs[1:-2:2]):
        for slot in range(mine.shape[0]):
            error[n] = ((mine[slot] + got[slot] - wanted[at + n]) / rows).astype(error.dtype)
            n += 1


def wanted_kernel(where, *refs, slots):
    table, wanted = refs[-2:]
    count = len(slots)
    targets = [ref[k : k + 1] for ref in refs[:-2] for k in range(ref.shape[0])]
    candidates = lax.broadcasted_iota(jnp.int32, (table.shape[0], wanted.shape[1]), 0)
    for i, (first, second) in enumerate(slots):
        offset = jnp.where(where[1] >> 1 == 1, second % count, first % count)
        place = replica_at(where[0], offset, count) ^ where[0]
        chosen = targets[0]
        for k in range(1, count):
            chosen = jnp.where(place == k, targets[k], chosen)
        hot = (candidates == chosen).astype(table.dtype)
        wanted[i] = lax.dot_general(
            hot, table[...], (((0,), (0,)), ((), ())), preferred_element_type=jnp.float32
        )


def ring_path(inputs, weight, table, targets):
    count = lax.axis_size("rep")
    rows = inputs.shape[0]
    features, columns = weight.shape
    quarter = rows // 4
    right = []
    left = []
    for i in range(count):
        ends = [2 * r if r < count // 2 else 2 * (count - 1 - r) + 1 for r in (i, (i + 1) % count)]
        right.append((ends[0], ends[1]))
        left.append((ends[1], ends[0]))
    far = count // 2
    where = jnp.stack([lax.axis_index("rep"), lax.axis_index("shard")])

    from_left = [[inputs[: rows // 2], inputs[rows // 2 :]]]
    from_right = [from_left[0]]
    for step in range(1, far + 1):
        last = step == far
        a = lax.ppermute(from_left[-1][0], "rep", right)
        d = lax.ppermute(from_right[-1][1], "rep", left)
        b = None if last else lax.ppermute(from_left[-1][1], "rep", right)
        c = None if last else lax.ppermute(from_right[-1][0], "rep", left)
        from_left.append([a, b])
        from_right.append([c, d])
    halves = {0: from_left[0], far: [from_left[far][0], from_right[far][1]]}
    for step in range(1, far):
        halves[-step] = from_left[step]
        halves[step] = from_right[step]
    phases = [[(0, 0)]]
    phases += [[(-step, step), (step, -step)] for step in range(1, far - 1)]
    phases += [[(1 - far, far - 1)], [(far - 1, 1 - far)], [(far, far)]]
    slots = tuple(slot for phase in phases for slot in phase)
    joined = [[0, 1]] + [[m] for m in range(2, far - 1)] + [[far - 1, far], [far + 1]]
    groups = [[0, -1, 1]] + [[-step, step] for step in range(2, far)] + [[far]]
    offsets = tuple(offset for group in groups for offset in group)

    pieces = [targets[None]]
    for i in range(count.bit_length() - 1):
        block = pieces[0]
        if i:
            shape = ((1 << i, quarter), targets.dtype)
            (block,) = local_call(join_kernel, (shape,), where, *pieces)
        pieces.append(lax.ppermute(block, "rep", [(r, r ^ 1 << i) for r in range(count)]))
    wanted = pl.pallas_call(
        functools.partial(wanted_kernel, slots=slots),
        grid_spec=pltpu.PrefetchScalarGridSpec(
            num_scalar_prefetch=1,
            grid=(1,),
            in_specs=[pl.BlockSpec(piece.shape, lambda i, where: (0, 0)) for piece in pieces]
            + [pl.BlockSpec((table.shape[0], columns), lambda i, where: (0, where[0]))],
            out_specs=pl.BlockSpec((count, quarter, columns), lambda i, where: (0, 0, 0)),
        ),
        out_shape=jax.ShapeDtypeStruct((count, quarter, columns), jnp.float32),
        compiler_params=pltpu.CompilerParams(vmem_limit_bytes=8 * 2**20),
        name="wanted",
    )(where, *pieces, table)

    swap_core = [(i, i ^ 1) for i in range(4)]
    swap_y = [(i, i ^ 2) for i in range(4)]
    (weight_b,) = local_call(cast_kernel, ((weight.shape, jnp.bfloat16),), where, weight)
    weight_other = lax.ppermute(weight_b, "shard", swap_core)
    summed = []
    for phase in phases:
        part = ((len(phase), quarter, columns), jnp.float32)
        xs = [halves[slot[half]][half] for slot in phase for half in range(2)]
        outgoing = xs
        if len(phase) > 1:
            shape = ((len(xs), quarter, features), inputs.dtype)
            outgoing = local_call(pick_kernel, (shape,), where, *xs)
        others = [lax.ppermute(x, "shard", swap_core) for x in outgoing]
        keep, send = local_call(
            outputs_kernel, (part, part), where, *xs, *others, weight_b, weight_other
        )
        summed += [(keep, lax.ppermute(send, "shard", swap_y))]

    errors = []
    errors_at = {}
    at = 0
    for m, members in enumerate(joined):
        mine = [slot for phase in members for slot in phases[phase]]
        for n, ends in enumerate(mine):
            errors_at[ends[0], 0] = (m, n)
            errors_at[ends[1], 1] = (m, n)
        (error,) = local_call(
            functools.partial(error_kernel, at=at, rows=rows),
            (((len(mine), quarter, columns), jnp.bfloat16),),
            where,
            *[part for phase in members for part in summed[phase]],
            wanted,
        )
        across = lax.ppermute(error, "shard", swap_y)
        other = lax.ppermute(error, "shard", swap_core)
        errors.append((error, across, other, lax.ppermute(across, "shard", swap_core)))
        at += len(mine)

    grads = []
    sums = []
    pairs = []
    for m, group in enumerate(groups):
        olds = len(grads)
        needed = sorted({errors_at[offset, half][0] for offset in group for half in range(2)})
        blocks = tuple(
            tuple((needed.index(errors_at[offset, half][0]), errors_at[offset, half][1]) for half in range(2))
            for offset in group
        )
        fresh = [(i, olds + n) for n in range(len(group)) for i in range(olds + n + 1)]
        pairs += fresh
        last = m == len(groups) - 1
        made = local_call(
            functools.partial(
                grad_kernel,
                blocks=blocks,
                phases=len(needed),
                olds=olds,
                pairs_of=tuple(pairs) if last else None,
                offsets=offsets if last else None,
            ),
            ((weight.shape, jnp.float32),) * len(group)
            + (((8, 128) if last else (len(fresh), 8, 128), jnp.float32),),
            where,
            *[halves[offset][half] for offset in group for half in range(2)],
            *[part for phase in needed for part in errors[phase]],
            *grads,
            *(sums if last else ()),
        )
        grads = grads + list(made[: len(group)])
        sums.append(made[len(group)])

    products = sums[-1]
    products = products + lax.ppermute(products, "shard", swap_core)
    products = products + lax.ppermute(products, "shard", swap_y)
    bit = 1
    while bit < count:
        products = products + lax.ppermute(products, "rep", [(i, i ^ bit) for i in range(count)])
        bit *= 2
    parts = 8
    smem = pl.BlockSpec(memory_space=pltpu.SMEM)
    vmem = pl.BlockSpec(memory_space=pltpu.VMEM)
    block = jax.ShapeDtypeStruct((features, columns), jnp.float32)
    return pl.pallas_call(
        functools.partial(combine_kernel, offsets=offsets, parts=parts),
        in_specs=[smem, smem] + [vmem] * (1 + count),
        out_specs=[pl.BlockSpec(memory_space=pltpu.HBM)] * 2,
        out_shape=[block] * 2,
        scratch_shapes=[pltpu.VMEM(block.shape, block.dtype)] * 2 + [pltpu.SemaphoreType.DMA((2, parts))],
        compiler_params=pltpu.CompilerParams(vmem_limit_bytes=12 * 2**20),
        name="combine",
    )(where, products, weight, *grads)


def gather_path(inputs, weight, table, targets):
    count = lax.axis_size("rep")
    rows = inputs.shape[0]
    features, columns = weight.shape
    rep = lax.axis_index("rep")
    all_inputs = lax.all_gather(inputs, "rep", axis=0, tiled=True)
    all_targets = lax.all_gather(targets, "rep", axis=0, tiled=False)
    partial = jnp.dot(all_inputs, weight.astype(jnp.bfloat16), preferred_element_type=jnp.float32)
    outputs = lax.psum_scatter(
        partial.reshape(count, rows, columns), "shard", scatter_dimension=1, tiled=True
    )
    table_columns = lax.dynamic_slice(table, (0, rep * columns), (table.shape[0], columns))
    wanted = table_columns[all_targets].astype(jnp.float32)
    error = ((outputs - wanted) / rows).astype(jnp.bfloat16)
    errors = lax.all_gather(error, "shard", axis=1, tiled=True)
    grads = lax.dot_general(
        all_inputs.reshape(count, rows, features),
        errors,
        (((1,), (1,)), ((0,), (0,))),
        preferred_element_type=jnp.float32,
    )
    products = lax.dot_general(
        grads, grads, (((1, 2), (1, 2)), ((), ())), precision=lax.Precision.HIGHEST
    )
    products = lax.psum(products, ("rep", "shard"))
    weights = jnp.stack(tree_weights(lambda a, b: products[a, b], count))
    combined = jnp.sum(weights[:, None, None] * grads, axis=0)
    return combined, weight - step_size * combined


def solution(mesh):
    count, shards = mesh.shape["rep"], mesh.shape["shard"]
    ring = shards == 4 and count == 8

    def on_device(inputs, weight, table, targets):
        if ring:
            return tuple(ring_path(inputs, weight, table, targets))
        return gather_path(inputs, weight, table, targets)

    in_specs = (P("rep", "shard"), P("shard", "rep"), P(), P(("rep", "shard")))
    out_specs = (P("shard", "rep"), P("shard", "rep"))
    return jax.shard_map(
        on_device, mesh=mesh, in_specs=in_specs, out_specs=out_specs, check_vma=False
    )
```
